8 devices in a mesh: data: 1 (over z), tensor: 8 (over y, x, core).
Axes of the slice: x: 2, y: 2, z: 1, core: 2. Of those that a mesh axis runs over, the one named last changes fastest.
Arguments:
- token_ids: int32 [32768], P(('data', 'tensor'))
- emb_table: bfloat16 [151936, 896], P('tensor')
- norm_gain: bfloat16 [896], replicated
- w_up: bfloat16 [896, 4864], P(None, 'tensor')
- w_down: bfloat16 [4864, 896], P('tensor')
- grad_out: bfloat16 [32768, 896], P(('data', 'tensor'))
Outputs:
- output 1: bfloat16 [32768, 896], P(('data', 'tensor'))
- output 2: float32 [151936, 896], P(('data', 'tensor'))
- output 3: float32 [896, 4864], P('data', 'tensor')
- output 4: float32 [4864, 896], P(('data', 'tensor'))
All inputs are finite; a program needn't handle non-finite values.
Results may differ from the reference program's by a relative error of at most 0.00554826.
Values are sent between devices in bfloat16 or wider.
A program may use at most 1 GiB of HBM per device.

```python
import math
import jax
import jax.numpy as jnp
from jax import lax

VOCAB_SIZE = 151936
MODEL_DIM = 896
FFN_DIM = 4864
TOKENS = 32768
HOT_IDS = 64
EPS = 1e-6
ROW_BLOCK = math.gcd(TOKENS, 2048)
NUM_BLOCKS = TOKENS // ROW_BLOCK


def draw_ids(key):
    key_uni, key_table, key_pick, key_coin = jax.random.split(key, 4)
    uniform_ids = jax.random.randint(key_uni, (TOKENS,), 0, VOCAB_SIZE)
    hot_table = jax.random.randint(key_table, (HOT_IDS,), 0, VOCAB_SIZE)
    hot_ids = hot_table[jax.random.randint(key_pick, (TOKENS,), 0, HOT_IDS)]
    coin_flip = jax.random.randint(key_coin, (TOKENS,), 0, 2)
    token_ids = jnp.where(coin_flip == 0, uniform_ids, hot_ids)
    token_ids = token_ids.at[0].set(0).at[TOKENS - 1].set(VOCAB_SIZE - 1)
    return token_ids.astype(jnp.int32)


def setup_inputs(seed: int = 0, part: int = 0) -> dict:
    shared_key, part_root = jax.random.split(jax.random.key(seed))
    key_emb, key_gain, key_up, key_down = jax.random.split(shared_key, 4)
    key_ids, key_grad = jax.random.split(jax.random.fold_in(part_root, part))
    emb_table = jax.random.normal(key_emb, (VOCAB_SIZE, MODEL_DIM), jnp.float32)
    norm_gain = 1.0 + 0.4 * jax.random.normal(key_gain, (MODEL_DIM,), jnp.float32)
    w_up = jax.random.normal(key_up, (MODEL_DIM, FFN_DIM), jnp.float32) * MODEL_DIM ** -0.5
    w_down = jax.random.normal(key_down, (FFN_DIM, MODEL_DIM), jnp.float32) * FFN_DIM ** -0.5
    grad_out = jax.random.normal(key_grad, (TOKENS, MODEL_DIM), jnp.float32)
    return {
        'token_ids': draw_ids(key_ids),
        'emb_table': emb_table.astype(jnp.bfloat16),
        'norm_gain': norm_gain.astype(jnp.bfloat16),
        'w_up': w_up.astype(jnp.bfloat16),
        'w_down': w_down.astype(jnp.bfloat16),
        'grad_out': grad_out.astype(jnp.bfloat16),
    }


def rms_norm(x_rows, gain_f):
    inv_rms = lax.rsqrt(jnp.mean(x_rows * x_rows, axis=-1, keepdims=True) + EPS)
    return x_rows * inv_rms * gain_f


def gelu_tanh(values):
    return jax.nn.gelu(values, approximate=True)


def reference(token_ids, emb_table, norm_gain, w_up, w_down, grad_out):
    gain_f = norm_gain.astype(jnp.float32)
    x_rows = jnp.take(emb_table, token_ids, axis=0)
    x_blocks = x_rows.reshape(NUM_BLOCKS, ROW_BLOCK, MODEL_DIM)
    grad_blocks = grad_out.reshape(NUM_BLOCKS, ROW_BLOCK, MODEL_DIM)

    def block_step(acc_pair, block_in):
        acc_up, acc_down = acc_pair
        x_blk = block_in[0].astype(jnp.float32)
        grad_blk = block_in[1]
        normed_f, norm_back = jax.vjp(lambda x_in: rms_norm(x_in, gain_f), x_blk)
        normed = normed_f.astype(jnp.bfloat16)
        pre_act = jnp.dot(normed, w_up, preferred_element_type=jnp.float32).astype(jnp.bfloat16)
        act_f, gelu_back = jax.vjp(gelu_tanh, pre_act.astype(jnp.float32))
        hidden = act_f.astype(jnp.bfloat16)
        y_blk = jnp.dot(hidden, w_down, preferred_element_type=jnp.float32)
        out_blk = (x_blk + y_blk).astype(jnp.bfloat16)
        d_hidden = jnp.dot(grad_blk, w_down.T, preferred_element_type=jnp.float32)
        d_pre = gelu_back(d_hidden)[0].astype(jnp.bfloat16)
        acc_down = acc_down + jnp.dot(hidden.T, grad_blk, preferred_element_type=jnp.float32)
        acc_up = acc_up + jnp.dot(normed.T, d_pre, preferred_element_type=jnp.float32)
        d_norm = jnp.dot(d_pre, w_up.T, preferred_element_type=jnp.float32)
        dx_blk = (grad_blk.astype(jnp.float32) + norm_back(d_norm)[0]).astype(jnp.bfloat16)
        return (acc_up, acc_down), (out_blk, dx_blk)

    zero_acc = (jnp.zeros((MODEL_DIM, FFN_DIM), jnp.float32), jnp.zeros((FFN_DIM, MODEL_DIM), jnp.float32))
    grads, outs = lax.scan(block_step, zero_acc, (x_blocks, grad_blocks))
    out = outs[0].reshape(TOKENS, MODEL_DIM)
    d_x = outs[1].reshape(TOKENS, MODEL_DIM).astype(jnp.float32)
    d_emb = jax.ops.segment_sum(d_x, token_ids, num_segments=VOCAB_SIZE)
    return (out, d_emb, grads[0], grads[1])
```

```python
import jax
import jax.numpy as jnp
from jax import lax
from jax.sharding import PartitionSpec as P

EPS = 1e-6


def rms_norm(x_rows, gain_f):
    inv_rms = lax.rsqrt(jnp.mean(x_rows * x_rows, axis=-1, keepdims=True) + EPS)
    return x_rows * inv_rms * gain_f


def gelu_tanh(values):
    return jax.nn.gelu(values, approximate=True)


def contract_last(left_op, right_op):
    return lax.dot_general(left_op, right_op, (((1,), (1,)), ((), ())), preferred_element_type=jnp.float32)


def contract_first(left_op, right_op):
    return lax.dot_general(left_op, right_op, (((0,), (0,)), ((), ())), preferred_element_type=jnp.float32)


def matmul(left_op, right_op):
    return jnp.dot(left_op, right_op, preferred_element_type=jnp.float32)


def solution(mesh):
    tok_spec = P(('data', 'tensor'))
    row_spec = P(('data', 'tensor'), None)

    def local_step(token_ids, emb_shard, norm_gain, w_up, w_down, grad_out):
        vocab_local = emb_shard.shape[0]
        offset = lax.axis_index('tensor') * vocab_local
        w_up_t = lax.all_gather(w_up.T, 'tensor', tiled=True)
        w_dn = lax.all_gather(w_down, 'tensor', tiled=True)
        ids_all = lax.all_gather(token_ids, 'tensor', tiled=True)
        rel_ids = ids_all - offset
        is_owned = (rel_ids >= 0) & (rel_ids < vocab_local)
        looked_up = jnp.take(emb_shard, jnp.clip(rel_ids, 0, vocab_local - 1), axis=0)
        emb_part = jnp.where(is_owned[:, None], looked_up, jnp.zeros((), looked_up.dtype))
        x_local = lax.psum_scatter(emb_part, 'tensor', scatter_dimension=0, tiled=True)
        x_f = x_local.astype(jnp.float32)
        gain_f = norm_gain.astype(jnp.float32)
        normed_f, norm_back = jax.vjp(lambda x_in: rms_norm(x_in, gain_f), x_f)
        normed = normed_f.astype(jnp.bfloat16)
        pre_act = contract_last(normed, w_up_t).astype(jnp.bfloat16)
        act_f, gelu_back = jax.vjp(gelu_tanh, pre_act.astype(jnp.float32))
        hidden = act_f.astype(jnp.bfloat16)
        d_w_down = lax.psum_scatter(contract_first(hidden, grad_out), 'tensor', scatter_dimension=0, tiled=True)
        d_hidden = contract_last(grad_out, w_dn)
        d_pre = gelu_back(d_hidden)[0].astype(jnp.bfloat16)
        d_norm = matmul(d_pre, w_up_t)
        dx_local = (grad_out.astype(jnp.float32) + norm_back(d_norm)[0]).astype(jnp.bfloat16)
        d_w_up = lax.psum_scatter(contract_first(d_pre, normed), 'tensor', scatter_dimension=0, tiled=True).T
        out_local = (x_f + matmul(hidden, w_dn)).astype(jnp.bfloat16)
        dx_all = lax.all_gather(dx_local, 'tensor', tiled=True)
        seg_ids = jnp.where(is_owned, rel_ids, vocab_local)
        d_emb = jax.ops.segment_sum(dx_all.astype(jnp.float32), seg_ids, num_segments=vocab_local + 1)[:vocab_local]
        return out_local, d_emb, d_w_up, d_w_down

    return jax.shard_map(
        local_step,
        mesh=mesh,
        in_specs=(tok_spec, P('tensor', None), P(None), P(None, 'tensor'), P('tensor', None), row_spec),
        out_specs=(row_spec, row_spec, P('data', 'tensor'), row_spec),
        check_vma=False,
    )
```

```python
import functools
import math
import jax
import jax.numpy as jnp
from jax import lax
from jax.experimental import pallas as pl
from jax.experimental.pallas import tpu as pltpu
from jax.sharding import PartitionSpec as P

EPS = 1e-6
BIG = 2 ** 30
N_DUP = 48
N_ONE = 336
N_REQ = N_DUP + N_ONE
GROUP = 64
ROWS = 8
TOK_BLOCK = 512
V_BLOCK = 256
WIN = 32
F_CHUNK = 256
GELU_A = (2 / math.pi) ** 0.5
GELU_B = 0.044715
F32 = jnp.float32
BF16 = jnp.bfloat16


def rms_norm(x_rows, gain_f):
    inv_rms = lax.rsqrt(jnp.mean(x_rows * x_rows, axis=-1, keepdims=True) + EPS)
    return x_rows * inv_rms * gain_f


def contract_last(left_op, right_op):
    return lax.dot_general(left_op, right_op, (((1,), (1,)), ((), ())), preferred_element_type=F32)


def contract_first(left_op, right_op):
    return lax.dot_general(left_op, right_op, (((0,), (0,)), ((), ())), preferred_element_type=F32)


def matmul(left_op, right_op):
    return jnp.dot(left_op, right_op, preferred_element_type=F32)


def route_kernel(me_ref, rnd_ref, ids_ref, out_ref, *, n_peer, vocab_local):
    s = ids_ref[...]
    n_row, n_lane = s.shape
    row = lax.broadcasted_iota(jnp.int32, s.shape, 0)
    lane = lax.broadcasted_iota(jnp.int32, s.shape, 1)
    back = pltpu.roll(s, 1, 1)
    back = jnp.where(lane == 0, pltpu.roll(back, 1, 0), back)
    ahead = pltpu.roll(s, n_lane - 1, 1)
    ahead = jnp.where(lane == n_lane - 1, pltpu.roll(ahead, n_row - 1, 0), ahead)
    is_first, is_last = row + lane == 0, row * n_lane + lane == n_row * n_lane - 1
    starts = (s != back) | is_first
    repeats = (s == ahead) & ~is_last
    owner = jnp.zeros_like(s)
    for d in range(1, n_peer):
        owner += (s >= d * vocab_local).astype(jnp.int32)
    up_to = (lax.broadcasted_iota(jnp.int32, (n_lane, n_lane), 0)
             <= lax.broadcasted_iota(jnp.int32, (n_lane, n_lane), 1)).astype(F32).astype(BF16)
    above = (lax.broadcasted_iota(jnp.int32, (n_row, n_row), 1)
             < lax.broadcasted_iota(jnp.int32, (n_row, n_row), 0)).astype(F32).astype(BF16)
    slot = jnp.full_like(s, -1)
    need = jnp.zeros((1, 1), F32)
    place = (owner ^ me_ref[0]) * N_REQ
    for flag, cap, shift in ((starts & repeats, N_DUP, 0), (starts & ~repeats, N_ONE, N_DUP)):
        mark = flag.astype(F32)
        incl = matmul(mark.astype(BF16), up_to)
        total = jnp.broadcast_to(incl[:, n_lane - 1:], s.shape)
        pos = incl - mark + matmul(above, total.astype(BF16))
        for d in range(1, n_peer):
            here = jnp.where(owner == d - 1, mark, 0.0)
            pos -= jnp.where(owner >= d, jnp.sum(here, keepdims=True), 0.0)
        trip = jnp.floor((pos + 0.5) / cap)
        need = jnp.maximum(need, jnp.max(jnp.where(flag, trip + 1.0, 0.0), keepdims=True))
        rel = pos.astype(jnp.int32) - rnd_ref[0] * cap
        slot = jnp.where(flag & (rel >= 0) & (rel < cap), place + shift + rel, slot)
    group, spot = slot >> 7, slot & 127
    spot_t = spot.astype(F32).T
    n_group = n_peer * N_REQ // 128
    group_iota = lax.broadcasted_iota(jnp.int32, (n_group, n_lane), 0)
    lane_sq = lax.broadcasted_iota(jnp.int32, (n_lane, n_lane), 1).astype(F32)
    parts = [(s & 63) + 1, (s >> 6) & 63, s >> 12]
    acc = jnp.zeros((3 * n_group, n_lane), F32)
    for a in range(n_row):
        at = group_iota == group[a:a + 1, :]
        left = jnp.concatenate([jnp.where(at, part[a:a + 1, :].astype(F32), 0.0) for part in parts], axis=0)
        right = (lane_sq == spot_t[:, a:a + 1]).astype(F32)
        acc += matmul(left.astype(BF16), right.astype(BF16))
    got = acc.astype(jnp.int32)
    got = got[:n_group] + got[n_group:2 * n_group] * 64 + got[2 * n_group:] * 4096 - 1
    rows = N_REQ // 128
    for k in range(n_peer):
        out_ref[k, :rows, :] = got[k * rows:(k + 1) * rows]
        out_ref[k, rows:, :] = jnp.broadcast_to(need.astype(jnp.int32), (8 - rows, n_lane))


def route(me, rnd, sorted_ids, n_peer, vocab_local):
    smem = pl.BlockSpec(memory_space=pltpu.SMEM)
    whole = pl.BlockSpec(memory_space=pltpu.VMEM)
    return pl.pallas_call(
        functools.partial(route_kernel, n_peer=n_peer, vocab_local=vocab_local),
        out_shape=jax.ShapeDtypeStruct((n_peer, 8, 128), jnp.int32),
        in_specs=[smem, smem, whole],
        out_specs=whole,
        cost_estimate=pl.CostEstimate(flops=10 ** 9, bytes_accessed=10 ** 5, transcendentals=0),
        name='route',
    )(me.reshape(1), rnd.reshape(1), sorted_ids)


def flipped(x, k):
    for bit in (1, 2, 4):
        if k & bit:
            x = x + bit - 2 * bit * ((x // bit) % 2)
    return x


def swap_kernel(mine_ref, theirs_ref, send_sem, recv_sem, *, n_peer):
    me = lax.axis_index('tensor')
    barrier = pltpu.get_barrier_semaphore()
    for k in range(1, n_peer):
        pl.semaphore_signal(barrier, inc=1, device_id={'tensor': flipped(me, k)}, device_id_type=pl.DeviceIdType.MESH)
    pl.semaphore_wait(barrier, n_peer - 1)
    copies = []
    for k in range(1, n_peer):
        copy = pltpu.make_async_remote_copy(
            src_ref=mine_ref.at[k], dst_ref=theirs_ref.at[k], send_sem=send_sem.at[k], recv_sem=recv_sem.at[k],
            device_id={'tensor': flipped(me, k)}, device_id_type=pl.DeviceIdType.MESH)
        copy.start()
        copies.append(copy)
    theirs_ref[0] = mine_ref[0]
    for copy in copies:
        copy.wait()


def swap_lists(mine):
    n_peer = mine.shape[0]
    whole = pl.BlockSpec(memory_space=pltpu.VMEM)
    return pl.pallas_call(
        functools.partial(swap_kernel, n_peer=n_peer),
        out_shape=jax.ShapeDtypeStruct(mine.shape, mine.dtype),
        in_specs=[whole],
        out_specs=whole,
        scratch_shapes=[pltpu.SemaphoreType.DMA((n_peer,)), pltpu.SemaphoreType.DMA((n_peer,))],
        compiler_params=pltpu.CompilerParams(collective_id=0, has_side_effects=True),
        name='swap_lists',
    )(mine)


def gather_kernel(idx_ref, sub_ref, emb_ref, *refs, n_out, depth):
    outs, (buf, sems) = refs[:n_out], refs[n_out:]
    per_out = N_REQ // GROUP
    steps = n_out * per_out

    def issue(step, slot):
        for i in range(GROUP):
            base = pl.multiple_of(idx_ref[step * GROUP + i], ROWS)
            pltpu.make_async_copy(emb_ref.at[pl.ds(base, ROWS), :], buf.at[slot, i], sems.at[slot]).start()

    for step in range(depth - 1):
        issue(step, step)
    lane = lax.broadcasted_iota(jnp.int32, (GROUP, GROUP * ROWS), 1)
    first = lax.broadcasted_iota(jnp.int32, (GROUP, GROUP * ROWS), 0) * ROWS

    for j in range(n_out):
        def body(i, carry, j=j):
            step = j * per_out + i
            slot = lax.rem(step, depth)

            @pl.when(step + depth - 1 < steps)
            def _():
                issue(step + depth - 1, lax.rem(step + depth - 1, depth))

            pltpu.make_async_copy(buf.at[slot], buf.at[slot], sems.at[slot]).wait()
            sub = sub_ref[pl.ds(pl.multiple_of(step * GROUP, GROUP), GROUP), :]
            pick = (lane == first + sub).astype(F32).astype(BF16)
            rows = matmul(pick, buf[slot].reshape(GROUP * ROWS, buf.shape[-1])).astype(BF16)
            outs[j][pl.ds(pl.multiple_of(i * GROUP, GROUP), GROUP), :] = rows
            return carry

        lax.fori_loop(0, per_out, body, 0)


def gather_rows(emb, idx, n_out):
    depth = 4
    dim = emb.shape[1]
    whole = pl.BlockSpec(memory_space=pltpu.VMEM)
    return pl.pallas_call(
        functools.partial(gather_kernel, n_out=n_out, depth=depth),
        out_shape=[jax.ShapeDtypeStruct((N_REQ, dim), BF16)] * n_out,
        in_specs=[pl.BlockSpec(memory_space=pltpu.SMEM), whole, pl.BlockSpec(memory_space=pl.ANY)],
        out_specs=[whole] * n_out,
        scratch_shapes=[
            pltpu.VMEM((depth, GROUP, ROWS, dim), BF16),
            pltpu.SemaphoreType.DMA((depth,)),
        ],
        cost_estimate=pl.CostEstimate(flops=14 * 10 ** 9, bytes_accessed=n_out * N_REQ * ROWS * dim * 2, transcendentals=0),
        name='gather_rows',
    )((idx // ROWS) * ROWS, (idx % ROWS)[:, None], emb)


def expand_kernel(ids_ref, gid_ref, gain_ref, *refs, n_peer, has_prev):
    recv = refs[:n_peer]
    x_ref, n_ref, table, hits = refs[-4:]

    @pl.when(pl.program_id(0) == 0)
    def _():
        for k in range(n_peer):
            table[k * N_REQ:(k + 1) * N_REQ, :] = recv[k][...]

    ids = ids_ref[...]
    for k in range(n_peer):
        hits[:, k * N_REQ:(k + 1) * N_REQ] = (ids == gid_ref[k:k + 1, :]).astype(F32).astype(BF16)
    acc = matmul(hits[...], table[...])
    if has_prev:
        acc += refs[n_peer][...].astype(F32)
    x_ref[...] = acc.astype(BF16)
    n_ref[...] = rms_norm(acc, gain_ref[...].astype(F32)).astype(BF16)


def expand_rows(ids_col, gid, gain_row, recv, prev=None):
    n_tok, dim = ids_col.shape[0], recv[0].shape[1]
    n_peer = len(recv)
    tok = pl.BlockSpec((TOK_BLOCK, dim), lambda i: (i, 0))
    whole = pl.BlockSpec(memory_space=pltpu.VMEM)
    extra = () if prev is None else (prev,)
    return pl.pallas_call(
        functools.partial(expand_kernel, n_peer=n_peer, has_prev=prev is not None),
        grid=(n_tok // TOK_BLOCK,),
        out_shape=[jax.ShapeDtypeStruct((n_tok, dim), BF16)] * 2,
        in_specs=[pl.BlockSpec((TOK_BLOCK, 1), lambda i: (i, 0)), whole, whole] + [whole] * n_peer + [tok] * len(extra),
        out_specs=[tok, tok],
        scratch_shapes=[pltpu.VMEM((n_peer * N_REQ, dim), BF16), pltpu.VMEM((TOK_BLOCK, n_peer * N_REQ), BF16)],
        cost_estimate=pl.CostEstimate(flops=22 * 10 ** 9, bytes_accessed=30 * 10 ** 6, transcendentals=0),
        name='expand_rows',
    )(ids_col, gid, gain_row, *recv, *extra)


def hidden_kernel(n_ref, grad_ref, w_up_ref, w_dn_ref, h_ref, du_ref, u_buf, dh_buf):
    n_chunk = w_up_ref.shape[0] // F_CHUNK

    def at(c):
        return pl.ds(c * F_CHUNK if isinstance(c, int) else pl.multiple_of(c * F_CHUNK, F_CHUNK), F_CHUNK)

    def dots(c, slot):
        u_buf[slot] = contract_last(n_ref[...], w_up_ref[at(c), :])
        dh_buf[slot] = contract_last(grad_ref[...], w_dn_ref[at(c), :])

    def act(c, slot):
        u = u_buf[slot].astype(BF16).astype(F32)
        sq = u * u
        half = 0.5 * jnp.tanh(u * (GELU_A + (GELU_A * GELU_B) * sq)) + 0.5
        h_ref[:, at(c)] = (u * half).astype(BF16)
        slope = half + u * (half - half * half) * (2 * GELU_A + (6 * GELU_A * GELU_B) * sq)
        du_ref[:, at(c)] = (dh_buf[slot] * slope).astype(BF16)

    dots(0, 0)

    def pair(i, carry):
        c = 2 * i
        dots(c + 1, 1)
        act(c, 0)
        dots(c + 2, 0)
        act(c + 1, 1)
        return carry

    lax.fori_loop(0, (n_chunk - 1) // 2, pair, 0)
    act(n_chunk - 1, 0)


def hidden_arrays(normed, grad_out, w_up_t, w_dn):
    n_tok, dim = normed.shape
    ffn = w_dn.shape[0]
    tok = pl.BlockSpec((TOK_BLOCK, dim), lambda i: (i, 0))
    wide = pl.BlockSpec((TOK_BLOCK, ffn), lambda i: (i, 0))
    whole = pl.BlockSpec(memory_space=pltpu.VMEM)
    return pl.pallas_call(
        hidden_kernel,
        grid=(n_tok // TOK_BLOCK,),
        out_shape=[jax.ShapeDtypeStruct((n_tok, ffn), BF16)] * 2,
        in_specs=[tok, tok, whole, whole],
        out_specs=[wide, wide],
        scratch_shapes=[pltpu.VMEM((2, TOK_BLOCK, F_CHUNK), F32)] * 2,
        compiler_params=pltpu.CompilerParams(vmem_limit_bytes=60 * 2 ** 20),
        cost_estimate=pl.CostEstimate(flops=4 * n_tok * dim * ffn, bytes_accessed=110 * 10 ** 6, transcendentals=n_tok * ffn),
        name='hidden_arrays',
    )(normed, grad_out, w_up_t, w_dn)


def combine_kernel(gid_ref, ids_ref, dx_ref, *refs, n_out):
    dups, ones, hits = refs[:n_out], refs[n_out:2 * n_out], refs[-1]
    n_tok = dx_ref.shape[0]
    step = 1024
    for j in range(n_out):
        gid = gid_ref[j * N_REQ:(j + 1) * N_REQ, :]
        for lo in range(0, n_tok, step):
            hits[:, lo:lo + step] = (gid == ids_ref[:, lo:lo + step]).astype(F32).astype(BF16)
        acc = matmul(hits[...], dx_ref[...])
        dups[j][...] = acc[:N_DUP]
        ones[j][...] = acc[N_DUP:].astype(BF16)


def combine_rows(gid_col, ids_row, d_x):
    n_tok, dim = d_x.shape
    n_out = gid_col.shape[0] // N_REQ
    whole = pl.BlockSpec(memory_space=pltpu.VMEM)
    outs = pl.pallas_call(
        functools.partial(combine_kernel, n_out=n_out),
        out_shape=[jax.ShapeDtypeStruct((N_DUP, dim), F32)] * n_out + [jax.ShapeDtypeStruct((N_ONE, dim), BF16)] * n_out,
        in_specs=[whole, whole, whole],
        out_specs=[whole] * (2 * n_out),
        scratch_shapes=[pltpu.VMEM((N_REQ, n_tok), BF16)],
        cost_estimate=pl.CostEstimate(flops=12 * 10 ** 9, bytes_accessed=12 * 10 ** 6, transcendentals=0),
        name='combine_rows',
    )(gid_col, ids_row, d_x)
    return outs[:n_out], outs[n_out:]


def table_kernel(off_one_ref, off_dup_ref, dup_id_ref, one_id_ref, *refs, n_peer, has_prev):
    ones = refs[:n_peer]
    dups = refs[n_peer:2 * n_peer]
    out_ref, rows_buf, id_buf = refs[-3:]
    blk = pl.program_id(0)
    base = blk * V_BLOCK
    starts, trips = [], jnp.int32(1)
    for k in range(n_peer):
        lo, hi = off_one_ref[k, blk], off_one_ref[k, blk + 1]
        start = (lo // 16) * 16
        starts.append(start)
        trips = jnp.maximum(trips, jnp.where(hi > lo, (hi - start + WIN - 1) // WIN, 0))
    pos = lax.broadcasted_iota(jnp.int32, (WIN, 1), 0)
    lane = lax.broadcasted_iota(jnp.int32, (n_peer * WIN, V_BLOCK), 1) + base

    def picked(it):
        for k in range(n_peer):
            want = starts[k] + it * WIN
            at = pl.multiple_of(jnp.minimum(want, N_ONE - WIN), 16)
            rows_buf[k * WIN:(k + 1) * WIN, :] = ones[k][pl.ds(at, WIN), :]
            window = one_id_ref[pl.ds(pl.multiple_of(k * N_ONE + at, 16), WIN), :]
            id_buf[k * WIN:(k + 1) * WIN, :] = jnp.where(pos + at >= want, window, -1)
        hit = (id_buf[...] == lane).astype(F32).astype(BF16)
        return contract_first(hit, rows_buf[...])

    out_ref[...] = refs[2 * n_peer][...] + picked(0) if has_prev else picked(0)

    def one_step(it, carry):
        out_ref[...] += picked(it)
        return carry

    lax.fori_loop(1, trips, one_step, 0)
    sub = lax.broadcasted_iota(jnp.int32, (8, 1), 0)
    for k in range(n_peer):
        def dup_step(j, carry, k=k):
            row = dup_id_ref[k, j] - base
            taken = dups[k][pl.ds(pl.multiple_of((j // 8) * 8, 8), 8), :]
            taken = jnp.sum(jnp.where(sub == lax.rem(j, 8), taken, 0.0), axis=0, keepdims=True)
            at = pl.ds(pl.multiple_of((row // 8) * 8, 8), 8)
            out_ref[at, :] += jnp.where(sub == lax.rem(row, 8), taken, 0.0)
            return carry

        lax.fori_loop(off_dup_ref[k, blk], off_dup_ref[k, blk + 1], dup_step, 0)


def table_grad(vocab_local, off_one, off_dup, dup_ids, one_ids, ones, dups, prev=None):
    n_peer, dim = len(ones), ones[0].shape[1]
    n_blk = pl.cdiv(vocab_local, V_BLOCK)
    smem = pl.BlockSpec(memory_space=pltpu.SMEM)
    whole = pl.BlockSpec(memory_space=pltpu.VMEM)
    rows = pl.BlockSpec((V_BLOCK, dim), lambda b: (b, 0))
    extra = () if prev is None else (prev,)
    return pl.pallas_call(
        functools.partial(table_kernel, n_peer=n_peer, has_prev=prev is not None),
        grid=(n_blk,),
        out_shape=jax.ShapeDtypeStruct((vocab_local, dim), F32),
        in_specs=[smem, smem, smem, whole] + [whole] * (2 * n_peer) + [rows] * len(extra),
        out_specs=rows,
        scratch_shapes=[
            pltpu.VMEM((n_peer * WIN, dim), BF16),
            pltpu.VMEM((n_peer * WIN, 1), jnp.int32),
        ],
        input_output_aliases={} if prev is None else {4 + 2 * n_peer: 0},
        cost_estimate=pl.CostEstimate(flops=25 * 10 ** 9, bytes_accessed=75 * 10 ** 6, transcendentals=0),
        name='table_grad',
    )(off_one, off_dup, dup_ids, one_ids, *ones, *dups, *extra)


def solution(mesh):
    tok_spec = P(('data', 'tensor'))
    row_spec = P(('data', 'tensor'), None)
    n_peer = mesh.shape['tensor']
    swaps = [[(i, i ^ k) for i in range(n_peer)] for k in range(n_peer)]

    def exchange(k, block):
        return block if k == 0 else lax.ppermute(block, 'tensor', swaps[k])

    def local_step(token_ids, emb_shard, norm_gain, w_up, w_down, grad_out):
        vocab_local = emb_shard.shape[0]
        n_tok = token_ids.shape[0]
        me = lax.axis_index('tensor')
        peers = me ^ jnp.arange(n_peer, dtype=jnp.int32)
        w_dn = lax.all_gather(w_down, 'tensor', tiled=True)
        w_up_t = lax.all_gather(w_up.T, 'tensor', tiled=True)

        sorted_ids = jnp.sort(token_ids).reshape(n_tok // 128, 128)
        rows_of = slice(0, N_REQ // 128)

        def asked(rnd):
            mine = route(me, jnp.int32(rnd), sorted_ids, n_peer, vocab_local)
            if isinstance(rnd, int):
                theirs = swap_lists(mine)
            else:
                theirs = jnp.stack([exchange(k, mine[k]) for k in range(n_peer)])
            rounds = jnp.max(theirs[:, -1, :])
            mine, theirs = (part[:, rows_of, :].reshape(n_peer, N_REQ) for part in (mine, theirs))
            return mine, jnp.where(theirs < 0, -1, theirs - me * vocab_local), rounds

        first = asked(0)
        rounds = first[2]
        halves = (range(n_peer // 2, n_peer), range(n_peer // 2))
        ids_col, ids_row = token_ids[:, None], token_ids[None, :]
        gain_row = norm_gain[None, :]

        def lookup(lists, prev=None):
            mine, theirs, _ = lists
            idx = jnp.clip(theirs, 0, vocab_local - 1)
            recv = {}
            for half in halves:
                blocks = gather_rows(emb_shard, idx[half.start:half.stop].reshape(-1), len(half))
                recv.update({k: exchange(k, block) for k, block in zip(half, blocks)})
            return expand_rows(ids_col, mine, gain_row, [recv[k] for k in range(n_peer)], prev)

        def lookup_step(carry):
            rnd, x_prev, _ = carry
            x_new, n_new = lookup(asked(rnd), x_prev)
            return rnd + 1, x_new, n_new

        x_first, n_first = lookup(first)
        _, x_local, normed = lax.while_loop(lambda c: c[0] < rounds, lookup_step, (jnp.int32(1), x_first, n_first))

        x_f = x_local.astype(F32)
        gain_f = norm_gain.astype(F32)
        _, norm_back = jax.vjp(lambda x_in: rms_norm(x_in, gain_f), x_f)
        hidden, d_pre = hidden_arrays(normed, grad_out, w_up_t, w_dn)
        d_w_down = lax.psum_scatter(contract_first(hidden, grad_out), 'tensor', scatter_dimension=0, tiled=True)
        d_norm = matmul(d_pre, w_up_t)
        dx_local = (grad_out.astype(F32) + norm_back(d_norm)[0]).astype(BF16)
        d_w_up = lax.psum_scatter(contract_first(d_pre, normed), 'tensor', scatter_dimension=0, tiled=True).T
        out_local = (x_f + matmul(hidden, w_dn)).astype(BF16)

        def table(lists, prev=None):
            mine, theirs, _ = lists
            dups, ones = {}, {}
            for half in halves:
                gid_col = mine[half.start:half.stop].reshape(-1, 1)
                for k, dup, one in zip(half, *combine_rows(gid_col, ids_row, dx_local)):
                    ones[k], dups[k] = exchange(k, one), exchange(k, dup)
            ones, dups = ([part[k] for k in range(n_peer)] for part in (ones, dups))
            keys = jnp.where(theirs < 0, BIG, theirs)
            marks = jnp.arange(pl.cdiv(vocab_local, V_BLOCK) + 1, dtype=jnp.int32) * V_BLOCK
            offs = [jnp.sum(part[:, None, :] < marks[None, :, None], axis=-1, dtype=jnp.int32)
                    for part in (keys[:, :N_DUP], keys[:, N_DUP:])]
            return table_grad(vocab_local, offs[1], offs[0], theirs[:, :N_DUP],
                              theirs[:, N_DUP:].reshape(n_peer * N_ONE, 1), ones, dups, prev)

        def table_step(carry):
            rnd, prev = carry
            return rnd + 1, table(asked(rnd), prev)

        _, d_emb = lax.while_loop(lambda c: c[0] < rounds, table_step, (jnp.int32(1), table(first)))
        return out_local, d_emb, d_w_up, d_w_down

    return jax.shard_map(
        local_step,
        mesh=mesh,
        in_specs=(tok_spec, P('tensor', None), P(None), P(None, 'tensor'), P('tensor', None), row_spec),
        out_specs=(row_spec, row_spec, P('data', 'tensor'), row_spec),
        check_vma=False,
    )
```

```python
import functools
import math
import jax
import jax.numpy as jnp
from jax import lax
from jax.experimental import pallas as pl
from jax.experimental.pallas import tpu as pltpu
from jax.sharding import PartitionSpec as P

EPS = 1e-6
BIG = 2 ** 30
N_DUP = 48
N_ONE = 336
N_REQ = N_DUP + N_ONE
GROUP = 64
ROWS = 8
TOK_BLOCK = 512
V_BLOCK = 768
WIN = 32
F_CHUNK = 256
GELU_A = (2 / math.pi) ** 0.5
GELU_B = 0.044715
F32 = jnp.float32
BF16 = jnp.bfloat16


def rms_norm(x_rows, gain_f):
    inv_rms = lax.rsqrt(jnp.mean(x_rows * x_rows, axis=-1, keepdims=True) + EPS)
    return x_rows * inv_rms * gain_f


def contract_last(left_op, right_op):
    return lax.dot_general(left_op, right_op, (((1,), (1,)), ((), ())), preferred_element_type=F32)


def contract_first(left_op, right_op):
    return lax.dot_general(left_op, right_op, (((0,), (0,)), ((), ())), preferred_element_type=F32)


def matmul(left_op, right_op):
    return jnp.dot(left_op, right_op, preferred_element_type=F32)


def route_kernel(me_ref, rnd_ref, ids_ref, out_ref, *, n_peer, vocab_local):
    s = ids_ref[...]
    n_row, n_lane = s.shape
    row = lax.broadcasted_iota(jnp.int32, s.shape, 0)
    lane = lax.broadcasted_iota(jnp.int32, s.shape, 1)
    back = pltpu.roll(s, 1, 1)
    back = jnp.where(lane == 0, pltpu.roll(back, 1, 0), back)
    ahead = pltpu.roll(s, n_lane - 1, 1)
    ahead = jnp.where(lane == n_lane - 1, pltpu.roll(ahead, n_row - 1, 0), ahead)
    is_first, is_last = row + lane == 0, row * n_lane + lane == n_row * n_lane - 1
    starts = (s != back) | is_first
    repeats = (s == ahead) & ~is_last
    owner = jnp.zeros_like(s)
    for d in range(1, n_peer):
        owner += (s >= d * vocab_local).astype(jnp.int32)
    up_to = (lax.broadcasted_iota(jnp.int32, (n_lane, n_lane), 0)
             <= lax.broadcasted_iota(jnp.int32, (n_lane, n_lane), 1)).astype(F32).astype(BF16)
    above = (lax.broadcasted_iota(jnp.int32, (n_row, n_row), 1)
             < lax.broadcasted_iota(jnp.int32, (n_row, n_row), 0)).astype(F32).astype(BF16)
    slot = jnp.full_like(s, -1)
    need = jnp.zeros((1, 1), F32)
    place = (owner ^ me_ref[0]) * N_REQ
    for flag, cap, shift in ((starts & repeats, N_DUP, 0), (starts & ~repeats, N_ONE, N_DUP)):
        mark = flag.astype(F32)
        incl = matmul(mark.astype(BF16), up_to)
        total = jnp.broadcast_to(incl[:, n_lane - 1:], s.shape)
        pos = incl - mark + matmul(above, total.astype(BF16))
        for d in range(1, n_peer):
            here = jnp.where(owner == d - 1, mark, 0.0)
            pos -= jnp.where(owner >= d, jnp.sum(here, keepdims=True), 0.0)
        trip = jnp.floor((pos + 0.5) / cap)
        need = jnp.maximum(need, jnp.max(jnp.where(flag, trip + 1.0, 0.0), keepdims=True))
        rel = pos.astype(jnp.int32) - rnd_ref[0] * cap
        slot = jnp.where(flag & (rel >= 0) & (rel < cap), place + shift + rel, slot)
    group, spot = slot >> 7, slot & 127
    spot_t = spot.astype(F32).T
    n_group = n_peer * N_REQ // 128
    group_iota = lax.broadcasted_iota(jnp.int32, (n_group, n_lane), 0)
    lane_sq = lax.broadcasted_iota(jnp.int32, (n_lane, n_lane), 1).astype(F32)
    parts = [(s & 63) + 1, (s >> 6) & 63, s >> 12]
    acc = jnp.zeros((3 * n_group, n_lane), F32)
    for a in range(n_row):
        at = group_iota == group[a:a + 1, :]
        left = jnp.concatenate([jnp.where(at, part[a:a + 1, :].astype(F32), 0.0) for part in parts], axis=0)
        right = (lane_sq == spot_t[:, a:a + 1]).astype(F32)
        acc += matmul(left.astype(BF16), right.astype(BF16))
    got = acc.astype(jnp.int32)
    got = got[:n_group] + got[n_group:2 * n_group] * 64 + got[2 * n_group:] * 4096 - 1
    rows = N_REQ // 128
    for k in range(n_peer):
        out_ref[k, :rows, :] = got[k * rows:(k + 1) * rows]
        out_ref[k, rows:, :] = jnp.broadcast_to(need.astype(jnp.int32), (8 - rows, n_lane))


def route(me, rnd, sorted_ids, n_peer, vocab_local):
    smem = pl.BlockSpec(memory_space=pltpu.SMEM)
    whole = pl.BlockSpec(memory_space=pltpu.VMEM)
    return pl.pallas_call(
        functools.partial(route_kernel, n_peer=n_peer, vocab_local=vocab_local),
        out_shape=jax.ShapeDtypeStruct((n_peer, 8, 128), jnp.int32),
        in_specs=[smem, smem, whole],
        out_specs=whole,
        cost_estimate=pl.CostEstimate(flops=10 ** 9, bytes_accessed=10 ** 5, transcendentals=0),
        name='route',
    )(me.reshape(1), rnd.reshape(1), sorted_ids)


def flipped(x, k):
    for bit in (1, 2, 4):
        if k & bit:
            x = x + bit - 2 * bit * ((x // bit) % 2)
    return x


def swap_kernel(mine_ref, theirs_ref, send_sem, recv_sem, *, n_peer):
    me = lax.axis_index('tensor')
    barrier = pltpu.get_barrier_semaphore()
    for k in range(1, n_peer):
        pl.semaphore_signal(barrier, inc=1, device_id={'tensor': flipped(me, k)}, device_id_type=pl.DeviceIdType.MESH)
    pl.semaphore_wait(barrier, n_peer - 1)
    copies = []
    for k in range(1, n_peer):
        copy = pltpu.make_async_remote_copy(
            src_ref=mine_ref.at[k], dst_ref=theirs_ref.at[k], send_sem=send_sem.at[k], recv_sem=recv_sem.at[k],
            device_id={'tensor': flipped(me, k)}, device_id_type=pl.DeviceIdType.MESH)
        copy.start()
        copies.append(copy)
    theirs_ref[0] = mine_ref[0]
    for copy in copies:
        copy.wait()


def swap_lists(mine):
    n_peer = mine.shape[0]
    whole = pl.BlockSpec(memory_space=pltpu.VMEM)
    return pl.pallas_call(
        functools.partial(swap_kernel, n_peer=n_peer),
        out_shape=jax.ShapeDtypeStruct(mine.shape, mine.dtype),
        in_specs=[whole],
        out_specs=whole,
        scratch_shapes=[pltpu.SemaphoreType.DMA((n_peer,)), pltpu.SemaphoreType.DMA((n_peer,))],
        compiler_params=pltpu.CompilerParams(collective_id=0, has_side_effects=True),
        name='swap_lists',
    )(mine)


def gather_kernel(idx_ref, sub_ref, emb_ref, *refs, n_out, depth):
    outs, (buf, sems) = refs[:n_out], refs[n_out:]
    per_out = N_REQ // GROUP
    steps = n_out * per_out

    def issue(step, slot):
        for i in range(GROUP):
            base = pl.multiple_of(idx_ref[step * GROUP + i], ROWS)
            pltpu.make_async_copy(emb_ref.at[pl.ds(base, ROWS), :], buf.at[slot, i], sems.at[slot]).start()

    for step in range(depth - 1):
        issue(step, step)
    lane = lax.broadcasted_iota(jnp.int32, (GROUP, GROUP * ROWS), 1)
    first = lax.broadcasted_iota(jnp.int32, (GROUP, GROUP * ROWS), 0) * ROWS

    for j in range(n_out):
        def body(i, carry, j=j):
            step = j * per_out + i
            slot = lax.rem(step, depth)

            @pl.when(step + depth - 1 < steps)
            def _():
                issue(step + depth - 1, lax.rem(step + depth - 1, depth))

            pltpu.make_async_copy(buf.at[slot], buf.at[slot], sems.at[slot]).wait()
            sub = sub_ref[pl.ds(pl.multiple_of(step * GROUP, GROUP), GROUP), :]
            pick = (lane == first + sub).astype(F32).astype(BF16)
            rows = matmul(pick, buf[slot].reshape(GROUP * ROWS, buf.shape[-1])).astype(BF16)
            outs[j][pl.ds(pl.multiple_of(i * GROUP, GROUP), GROUP), :] = rows
            return carry

        lax.fori_loop(0, per_out, body, 0)


def gather_rows(emb, idx, n_out):
    depth = 4
    dim = emb.shape[1]
    whole = pl.BlockSpec(memory_space=pltpu.VMEM)
    return pl.pallas_call(
        functools.partial(gather_kernel, n_out=n_out, depth=depth),
        out_shape=[jax.ShapeDtypeStruct((N_REQ, dim), BF16)] * n_out,
        in_specs=[pl.BlockSpec(memory_space=pltpu.SMEM), whole, pl.BlockSpec(memory_space=pl.ANY)],
        out_specs=[whole] * n_out,
        scratch_shapes=[
            pltpu.VMEM((depth, GROUP, ROWS, dim), BF16),
            pltpu.SemaphoreType.DMA((depth,)),
        ],
        cost_estimate=pl.CostEstimate(flops=14 * 10 ** 9, bytes_accessed=n_out * N_REQ * ROWS * dim * 2, transcendentals=0),
        name='gather_rows',
    )((idx // ROWS) * ROWS, (idx % ROWS)[:, None], emb)


def expand_kernel(ids_ref, gid_ref, gain_ref, *refs, n_peer, has_prev):
    recv = refs[:n_peer]
    x_ref, n_ref, table, hits = refs[-4:]

    @pl.when(pl.program_id(0) == 0)
    def _():
        for k in range(n_peer):
            table[k * N_REQ:(k + 1) * N_REQ, :] = recv[k][...]

    ids = ids_ref[...]
    for k in range(n_peer):
        hits[:, k * N_REQ:(k + 1) * N_REQ] = (ids == gid_ref[k:k + 1, :]).astype(F32).astype(BF16)
    acc = matmul(hits[...], table[...])
    if has_prev:
        acc += refs[n_peer][...].astype(F32)
    x_ref[...] = acc.astype(BF16)
    n_ref[...] = rms_norm(acc, gain_ref[...].astype(F32)).astype(BF16)


def expand_rows(ids_col, gid, gain_row, recv, prev=None):
    n_tok, dim = ids_col.shape[0], recv[0].shape[1]
    n_peer = len(recv)
    tok = pl.BlockSpec((TOK_BLOCK, dim), lambda i: (i, 0))
    whole = pl.BlockSpec(memory_space=pltpu.VMEM)
    extra = () if prev is None else (prev,)
    return pl.pallas_call(
        functools.partial(expand_kernel, n_peer=n_peer, has_prev=prev is not None),
        grid=(n_tok // TOK_BLOCK,),
        out_shape=[jax.ShapeDtypeStruct((n_tok, dim), BF16)] * 2,
        in_specs=[pl.BlockSpec((TOK_BLOCK, 1), lambda i: (i, 0)), whole, whole] + [whole] * n_peer + [tok] * len(extra),
        out_specs=[tok, tok],
        scratch_shapes=[pltpu.VMEM((n_peer * N_REQ, dim), BF16), pltpu.VMEM((TOK_BLOCK, n_peer * N_REQ), BF16)],
        cost_estimate=pl.CostEstimate(flops=22 * 10 ** 9, bytes_accessed=30 * 10 ** 6, transcendentals=0),
        name='expand_rows',
    )(ids_col, gid, gain_row, *recv, *extra)


def hidden_kernel(n_ref, grad_ref, w_up_ref, w_dn_ref, h_ref, du_ref, u_buf, dh_buf):
    n_chunk = w_up_ref.shape[0] // F_CHUNK

    def at(c):
        return pl.ds(c * F_CHUNK if isinstance(c, int) else pl.multiple_of(c * F_CHUNK, F_CHUNK), F_CHUNK)

    def dots(c, slot):
        u_buf[slot] = contract_last(n_ref[...], w_up_ref[at(c), :])
        dh_buf[slot] = contract_last(grad_ref[...], w_dn_ref[at(c), :])

    def act(c, slot):
        u = u_buf[slot].astype(BF16).astype(F32)
        sq = u * u
        half = 0.5 * jnp.tanh(u * (GELU_A + (GELU_A * GELU_B) * sq)) + 0.5
        h_ref[:, at(c)] = (u * half).astype(BF16)
        slope = half + u * (half - half * half) * (2 * GELU_A + (6 * GELU_A * GELU_B) * sq)
        du_ref[:, at(c)] = (dh_buf[slot] * slope).astype(BF16)

    dots(0, 0)

    def pair(i, carry):
        c = 2 * i
        dots(c + 1, 1)
        act(c, 0)
        dots(c + 2, 0)
        act(c + 1, 1)
        return carry

    lax.fori_loop(0, (n_chunk - 1) // 2, pair, 0)
    act(n_chunk - 1, 0)


def hidden_arrays(normed, grad_out, w_up_t, w_dn):
    n_tok, dim = normed.shape
    ffn = w_dn.shape[0]
    tok = pl.BlockSpec((TOK_BLOCK, dim), lambda i: (i, 0))
    wide = pl.BlockSpec((TOK_BLOCK, ffn), lambda i: (i, 0))
    whole = pl.BlockSpec(memory_space=pltpu.VMEM)
    return pl.pallas_call(
        hidden_kernel,
        grid=(n_tok // TOK_BLOCK,),
        out_shape=[jax.ShapeDtypeStruct((n_tok, ffn), BF16)] * 2,
        in_specs=[tok, tok, whole, whole],
        out_specs=[wide, wide],
        scratch_shapes=[pltpu.VMEM((2, TOK_BLOCK, F_CHUNK), F32)] * 2,
        compiler_params=pltpu.CompilerParams(vmem_limit_bytes=60 * 2 ** 20),
        cost_estimate=pl.CostEstimate(flops=4 * n_tok * dim * ffn, bytes_accessed=110 * 10 ** 6, transcendentals=n_tok * ffn),
        name='hidden_arrays',
    )(normed, grad_out, w_up_t, w_dn)


def combine_kernel(gid_ref, ids_ref, dx_ref, *refs, n_out):
    dups, ones, hits = refs[:n_out], refs[n_out:2 * n_out], refs[-1]
    n_tok = dx_ref.shape[0]
    step = 1024
    for j in range(n_out):
        gid = gid_ref[j * N_REQ:(j + 1) * N_REQ, :]
        for lo in range(0, n_tok, step):
            hits[:, lo:lo + step] = (gid == ids_ref[:, lo:lo + step]).astype(F32).astype(BF16)
        acc = matmul(hits[...], dx_ref[...])
        dups[j][...] = acc[:N_DUP]
        ones[j][...] = acc[N_DUP:].astype(BF16)


def combine_rows(gid_col, ids_row, d_x):
    n_tok, dim = d_x.shape
    n_out = gid_col.shape[0] // N_REQ
    whole = pl.BlockSpec(memory_space=pltpu.VMEM)
    outs = pl.pallas_call(
        functools.partial(combine_kernel, n_out=n_out),
        out_shape=[jax.ShapeDtypeStruct((N_DUP, dim), F32)] * n_out + [jax.ShapeDtypeStruct((N_ONE, dim), BF16)] * n_out,
        in_specs=[whole, whole, whole],
        out_specs=[whole] * (2 * n_out),
        scratch_shapes=[pltpu.VMEM((N_REQ, n_tok), BF16)],
        cost_estimate=pl.CostEstimate(flops=12 * 10 ** 9, bytes_accessed=12 * 10 ** 6, transcendentals=0),
        name='combine_rows',
    )(gid_col, ids_row, d_x)
    return outs[:n_out], outs[n_out:]


def table_kernel(off_one_ref, off_dup_ref, dup_id_ref, one_id_ref, *refs, n_peer, has_prev):
    ones = refs[:n_peer]
    dups = refs[n_peer:2 * n_peer]
    out_ref, rows_buf, id_buf = refs[-3:]
    blk = pl.program_id(0)
    base = blk * V_BLOCK
    starts, trips = [], jnp.int32(1)
    for k in range(n_peer):
        lo, hi = off_one_ref[k, blk], off_one_ref[k, blk + 1]
        start = (lo // 16) * 16
        starts.append(start)
        trips = jnp.maximum(trips, jnp.where(hi > lo, (hi - start + WIN - 1) // WIN, 0))
    pos = lax.broadcasted_iota(jnp.int32, (WIN, 1), 0)
    lane = lax.broadcasted_iota(jnp.int32, (n_peer * WIN, V_BLOCK), 1) + base

    def picked(it):
        for k in range(n_peer):
            want = starts[k] + it * WIN
            at = pl.multiple_of(jnp.minimum(want, N_ONE - WIN), 16)
            rows_buf[k * WIN:(k + 1) * WIN, :] = ones[k][pl.ds(at, WIN), :]
            window = one_id_ref[pl.ds(pl.multiple_of(k * N_ONE + at, 16), WIN), :]
            id_buf[k * WIN:(k + 1) * WIN, :] = jnp.where(pos + at >= want, window, -1)
        hit = (id_buf[...] == lane).astype(F32).astype(BF16)
        return contract_first(hit, rows_buf[...])

    out_ref[...] = refs[2 * n_peer][...] + picked(0) if has_prev else picked(0)

    def one_step(it, carry):
        out_ref[...] += picked(it)
        return carry

    lax.fori_loop(1, trips, one_step, 0)
    sub = lax.broadcasted_iota(jnp.int32, (8, 1), 0)
    for k in range(n_peer):
        def dup_step(j, carry, k=k):
            row = dup_id_ref[k, j] - base
            taken = dups[k][pl.ds(pl.multiple_of((j // 8) * 8, 8), 8), :]
            taken = jnp.sum(jnp.where(sub == lax.rem(j, 8), taken, 0.0), axis=0, keepdims=True)
            at = pl.ds(pl.multiple_of((row // 8) * 8, 8), 8)
            out_ref[at, :] += jnp.where(sub == lax.rem(row, 8), taken, 0.0)
            return carry

        lax.fori_loop(off_dup_ref[k, blk], off_dup_ref[k, blk + 1], dup_step, 0)


def table_grad(vocab_local, off_one, off_dup, dup_ids, one_ids, ones, dups, prev=None):
    n_peer, dim = len(ones), ones[0].shape[1]
    n_blk = pl.cdiv(vocab_local, V_BLOCK)
    smem = pl.BlockSpec(memory_space=pltpu.SMEM)
    whole = pl.BlockSpec(memory_space=pltpu.VMEM)
    rows = pl.BlockSpec((V_BLOCK, dim), lambda b: (b, 0))
    extra = () if prev is None else (prev,)
    return pl.pallas_call(
        functools.partial(table_kernel, n_peer=n_peer, has_prev=prev is not None),
        grid=(n_blk,),
        out_shape=jax.ShapeDtypeStruct((vocab_local, dim), F32),
        in_specs=[smem, smem, smem, whole] + [whole] * (2 * n_peer) + [rows] * len(extra),
        out_specs=rows,
        scratch_shapes=[
            pltpu.VMEM((n_peer * WIN, dim), BF16),
            pltpu.VMEM((n_peer * WIN, 1), jnp.int32),
        ],
        input_output_aliases={} if prev is None else {4 + 2 * n_peer: 0},
        cost_estimate=pl.CostEstimate(flops=25 * 10 ** 9, bytes_accessed=75 * 10 ** 6, transcendentals=0),
        name='table_grad',
    )(off_one, off_dup, dup_ids, one_ids, *ones, *dups, *extra)


def solution(mesh):
    tok_spec = P(('data', 'tensor'))
    row_spec = P(('data', 'tensor'), None)
    n_peer = mesh.shape['tensor']
    swaps = [[(i, i ^ k) for i in range(n_peer)] for k in range(n_peer)]

    def exchange(k, block):
        return block if k == 0 else lax.ppermute(block, 'tensor', swaps[k])

    def local_step(token_ids, emb_shard, norm_gain, w_up, w_down, grad_out):
        vocab_local = emb_shard.shape[0]
        n_tok = token_ids.shape[0]
        me = lax.axis_index('tensor')
        peers = me ^ jnp.arange(n_peer, dtype=jnp.int32)
        w_dn = lax.all_gather(w_down, 'tensor', tiled=True)
        w_up_t = lax.all_gather(w_up.T, 'tensor', tiled=True)

        sorted_ids = jnp.sort(token_ids).reshape(n_tok // 128, 128)
        rows_of = slice(0, N_REQ // 128)

        def asked(rnd):
            mine = route(me, jnp.int32(rnd), sorted_ids, n_peer, vocab_local)
            if isinstance(rnd, int):
                theirs = swap_lists(mine)
            else:
                theirs = jnp.stack([exchange(k, mine[k]) for k in range(n_peer)])
            rounds = jnp.max(theirs[:, -1, :])
            mine, theirs = (part[:, rows_of, :].reshape(n_peer, N_REQ) for part in (mine, theirs))
            return mine, jnp.where(theirs < 0, -1, theirs - me * vocab_local), rounds

        first = asked(0)
        rounds = first[2]
        halves = (range(n_peer // 2, n_peer), range(n_peer // 2))
        ids_col, ids_row = token_ids[:, None], token_ids[None, :]
        gain_row = norm_gain[None, :]

        def lookup(lists, prev=None):
            mine, theirs, _ = lists
            idx = jnp.clip(theirs, 0, vocab_local - 1)
            recv = {}
            for half in halves:
                blocks = gather_rows(emb_shard, idx[half.start:half.stop].reshape(-1), len(half))
                recv.update({k: exchange(k, block) for k, block in zip(half, blocks)})
            return expand_rows(ids_col, mine, gain_row, [recv[k] for k in range(n_peer)], prev)

        def lookup_step(carry):
            rnd, x_prev, _ = carry
            x_new, n_new = lookup(asked(rnd), x_prev)
            return rnd + 1, x_new, n_new

        x_first, n_first = lookup(first)
        _, x_local, normed = lax.while_loop(lambda c: c[0] < rounds, lookup_step, (jnp.int32(1), x_first, n_first))

        x_f = x_local.astype(F32)
        gain_f = norm_gain.astype(F32)
        _, norm_back = jax.vjp(lambda x_in: rms_norm(x_in, gain_f), x_f)
        hidden, d_pre = hidden_arrays(normed, grad_out, w_up_t, w_dn)
        d_w_down = lax.psum_scatter(contract_first(hidden, grad_out), 'tensor', scatter_dimension=0, tiled=True)
        up_part, d_pre = lax.optimization_barrier((contract_first(d_pre, normed), d_pre))
        d_norm = matmul(d_pre, w_up_t)
        dx_local = (grad_out.astype(F32) + norm_back(d_norm)[0]).astype(BF16)
        d_w_up = lax.psum_scatter(up_part, 'tensor', scatter_dimension=0, tiled=True).T
        out_local = (x_f + matmul(hidden, w_dn)).astype(BF16)

        def table(lists, prev=None):
            mine, theirs, _ = lists
            dups, ones = {}, {}
            for half in halves:
                gid_col = mine[half.start:half.stop].reshape(-1, 1)
                for k, dup, one in zip(half, *combine_rows(gid_col, ids_row, dx_local)):
                    ones[k], dups[k] = exchange(k, one), exchange(k, dup)
            ones, dups = ([part[k] for k in range(n_peer)] for part in (ones, dups))
            keys = jnp.where(theirs < 0, BIG, theirs)
            marks = jnp.arange(pl.cdiv(vocab_local, V_BLOCK) + 1, dtype=jnp.int32) * V_BLOCK
            offs = [jnp.sum(part[:, None, :] < marks[None, :, None], axis=-1, dtype=jnp.int32)
                    for part in (keys[:, :N_DUP], keys[:, N_DUP:])]
            return table_grad(vocab_local, offs[1], offs[0], theirs[:, :N_DUP],
                              theirs[:, N_DUP:].reshape(n_peer * N_ONE, 1), ones, dups, prev)

        def table_step(carry):
            rnd, prev = carry
            return rnd + 1, table(asked(rnd), prev)

        _, d_emb = lax.while_loop(lambda c: c[0] < rounds, table_step, (jnp.int32(1), table(first)))
        return out_local, d_emb, d_w_up, d_w_down

    return jax.shard_map(
        local_step,
        mesh=mesh,
        in_specs=(tok_spec, P('tensor', None), P(None), P(None, 'tensor'), P('tensor', None), row_spec),
        out_specs=(row_spec, row_spec, P('data', 'tensor'), row_spec),
        check_vma=False,
    )
```

```python
import functools
import math
import jax
import jax.numpy as jnp
from jax import lax
from jax.experimental import pallas as pl
from jax.experimental.pallas import tpu as pltpu
from jax.sharding import PartitionSpec as P

EPS = 1e-6
BIG = 2 ** 30
N_DUP = 48
N_ONE = 336
N_REQ = N_DUP + N_ONE
GROUP = 64
ROWS = 8
TOK_BLOCK = 512
V_BLOCK = 768
WIN = 32
F_CHUNK = 256
GELU_A = (2 / math.pi) ** 0.5
GELU_B = 0.044715
F32 = jnp.float32
BF16 = jnp.bfloat16


def rms_norm(x_rows, gain_f):
    inv_rms = lax.rsqrt(jnp.mean(x_rows * x_rows, axis=-1, keepdims=True) + EPS)
    return x_rows * inv_rms * gain_f


def contract_last(left_op, right_op):
    return lax.dot_general(left_op, right_op, (((1,), (1,)), ((), ())), preferred_element_type=F32)


def contract_first(left_op, right_op):
    return lax.dot_general(left_op, right_op, (((0,), (0,)), ((), ())), preferred_element_type=F32)


def matmul(left_op, right_op):
    return jnp.dot(left_op, right_op, preferred_element_type=F32)


def route_kernel(me_ref, rnd_ref, ids_ref, out_ref, *, n_peer, vocab_local):
    s = ids_ref[...]
    n_row, n_lane = s.shape
    row = lax.broadcasted_iota(jnp.int32, s.shape, 0)
    lane = lax.broadcasted_iota(jnp.int32, s.shape, 1)
    back = pltpu.roll(s, 1, 1)
    back = jnp.where(lane == 0, pltpu.roll(back, 1, 0), back)
    ahead = pltpu.roll(s, n_lane - 1, 1)
    ahead = jnp.where(lane == n_lane - 1, pltpu.roll(ahead, n_row - 1, 0), ahead)
    is_first, is_last = row + lane == 0, row * n_lane + lane == n_row * n_lane - 1
    starts = (s != back) | is_first
    repeats = (s == ahead) & ~is_last
    owner = jnp.zeros_like(s)
    for d in range(1, n_peer):
        owner += (s >= d * vocab_local).astype(jnp.int32)
    up_to = (lax.broadcasted_iota(jnp.int32, (n_lane, n_lane), 0)
             <= lax.broadcasted_iota(jnp.int32, (n_lane, n_lane), 1)).astype(F32).astype(BF16)
    above = (lax.broadcasted_iota(jnp.int32, (n_row, n_row), 1)
             < lax.broadcasted_iota(jnp.int32, (n_row, n_row), 0)).astype(F32).astype(BF16)
    slot = jnp.full_like(s, -1)
    need = jnp.zeros((1, 1), F32)
    place = (owner ^ me_ref[0]) * N_REQ
    for flag, cap, shift in ((starts & repeats, N_DUP, 0), (starts & ~repeats, N_ONE, N_DUP)):
        mark = flag.astype(F32)
        incl = matmul(mark.astype(BF16), up_to)
        total = jnp.broadcast_to(incl[:, n_lane - 1:], s.shape)
        pos = incl - mark + matmul(above, total.astype(BF16))
        for d in range(1, n_peer):
            here = jnp.where(owner == d - 1, mark, 0.0)
            pos -= jnp.where(owner >= d, jnp.sum(here, keepdims=True), 0.0)
        trip = jnp.floor((pos + 0.5) / cap)
        need = jnp.maximum(need, jnp.max(jnp.where(flag, trip + 1.0, 0.0), keepdims=True))
        rel = pos.astype(jnp.int32) - rnd_ref[0] * cap
        slot = jnp.where(flag & (rel >= 0) & (rel < cap), place + shift + rel, slot)
    group, spot = slot >> 7, slot & 127
    spot_t = spot.astype(F32).T
    n_group = n_peer * N_REQ // 128
    group_iota = lax.broadcasted_iota(jnp.int32, (n_group, n_lane), 0)
    lane_sq = lax.broadcasted_iota(jnp.int32, (n_lane, n_lane), 1).astype(F32)
    parts = [(s & 63) + 1, (s >> 6) & 63, s >> 12]
    acc = jnp.zeros((3 * n_group, n_lane), F32)
    for a in range(n_row):
        at = group_iota == group[a:a + 1, :]
        left = jnp.concatenate([jnp.where(at, part[a:a + 1, :].astype(F32), 0.0) for part in parts], axis=0)
        right = (lane_sq == spot_t[:, a:a + 1]).astype(F32)
        acc += matmul(left.astype(BF16), right.astype(BF16))
    got = acc.astype(jnp.int32)
    got = got[:n_group] + got[n_group:2 * n_group] * 64 + got[2 * n_group:] * 4096 - 1
    rows = N_REQ // 128
    for k in range(n_peer):
        out_ref[k, :rows, :] = got[k * rows:(k + 1) * rows]
        out_ref[k, rows:, :] = jnp.broadcast_to(need.astype(jnp.int32), (8 - rows, n_lane))


def route(me, rnd, sorted_ids, n_peer, vocab_local):
    smem = pl.BlockSpec(memory_space=pltpu.SMEM)
    whole = pl.BlockSpec(memory_space=pltpu.VMEM)
    return pl.pallas_call(
        functools.partial(route_kernel, n_peer=n_peer, vocab_local=vocab_local),
        out_shape=jax.ShapeDtypeStruct((n_peer, 8, 128), jnp.int32),
        in_specs=[smem, smem, whole],
        out_specs=whole,
        cost_estimate=pl.CostEstimate(flops=10 ** 9, bytes_accessed=10 ** 5, transcendentals=0),
        name='route',
    )(me.reshape(1), rnd.reshape(1), sorted_ids)


def flipped(x, k):
    for bit in (1, 2, 4):
        if k & bit:
            x = x + bit - 2 * bit * ((x // bit) % 2)
    return x


def swap_kernel(mine_ref, theirs_ref, send_sem, recv_sem, *, n_peer):
    me = lax.axis_index('tensor')
    barrier = pltpu.get_barrier_semaphore()
    for k in range(1, n_peer):
        pl.semaphore_signal(barrier, inc=1, device_id={'tensor': flipped(me, k)}, device_id_type=pl.DeviceIdType.MESH)
    pl.semaphore_wait(barrier, n_peer - 1)
    copies = []
    for k in range(1, n_peer):
        copy = pltpu.make_async_remote_copy(
            src_ref=mine_ref.at[k], dst_ref=theirs_ref.at[k], send_sem=send_sem.at[k], recv_sem=recv_sem.at[k],
            device_id={'tensor': flipped(me, k)}, device_id_type=pl.DeviceIdType.MESH)
        copy.start()
        copies.append(copy)
    theirs_ref[0] = mine_ref[0]
    for copy in copies:
        copy.wait()


def swap_lists(mine):
    n_peer = mine.shape[0]
    whole = pl.BlockSpec(memory_space=pltpu.VMEM)
    return pl.pallas_call(
        functools.partial(swap_kernel, n_peer=n_peer),
        out_shape=jax.ShapeDtypeStruct(mine.shape, mine.dtype),
        in_specs=[whole],
        out_specs=whole,
        scratch_shapes=[pltpu.SemaphoreType.DMA((n_peer,)), pltpu.SemaphoreType.DMA((n_peer,))],
        compiler_params=pltpu.CompilerParams(collective_id=0, has_side_effects=True),
        name='swap_lists',
    )(mine)


def gather_kernel(idx_ref, sub_ref, emb_ref, *refs, n_out, depth):
    outs, (buf, sems) = refs[:n_out], refs[n_out:]
    per_out = N_REQ // GROUP
    steps = n_out * per_out

    def issue(step, slot):
        for i in range(GROUP):
            base = pl.multiple_of(idx_ref[step * GROUP + i], ROWS)
            pltpu.make_async_copy(emb_ref.at[pl.ds(base, ROWS), :], buf.at[slot, i], sems.at[slot]).start()

    for step in range(depth - 1):
        issue(step, step)
    lane = lax.broadcasted_iota(jnp.int32, (GROUP, GROUP * ROWS), 1)
    first = lax.broadcasted_iota(jnp.int32, (GROUP, GROUP * ROWS), 0) * ROWS

    for j in range(n_out):
        def body(i, carry, j=j):
            step = j * per_out + i
            slot = lax.rem(step, depth)

            @pl.when(step + depth - 1 < steps)
            def _():
                issue(step + depth - 1, lax.rem(step + depth - 1, depth))

            pltpu.make_async_copy(buf.at[slot], buf.at[slot], sems.at[slot]).wait()
            sub = sub_ref[pl.ds(pl.multiple_of(step * GROUP, GROUP), GROUP), :]
            pick = (lane == first + sub).astype(F32).astype(BF16)
            rows = matmul(pick, buf[slot].reshape(GROUP * ROWS, buf.shape[-1])).astype(BF16)
            outs[j][pl.ds(pl.multiple_of(i * GROUP, GROUP), GROUP), :] = rows
            return carry

        lax.fori_loop(0, per_out, body, 0)


def gather_rows(emb, idx, n_out):
    depth = 4
    dim = emb.shape[1]
    whole = pl.BlockSpec(memory_space=pltpu.VMEM)
    return pl.pallas_call(
        functools.partial(gather_kernel, n_out=n_out, depth=depth),
        out_shape=[jax.ShapeDtypeStruct((N_REQ, dim), BF16)] * n_out,
        in_specs=[pl.BlockSpec(memory_space=pltpu.SMEM), whole, pl.BlockSpec(memory_space=pl.ANY)],
        out_specs=[whole] * n_out,
        scratch_shapes=[
            pltpu.VMEM((depth, GROUP, ROWS, dim), BF16),
            pltpu.SemaphoreType.DMA((depth,)),
        ],
        cost_estimate=pl.CostEstimate(flops=14 * 10 ** 9, bytes_accessed=n_out * N_REQ * ROWS * dim * 2, transcendentals=0),
        name='gather_rows',
    )((idx // ROWS) * ROWS, (idx % ROWS)[:, None], emb)


def expand_kernel(ids_ref, gid_ref, gain_ref, *refs, n_peer, has_prev):
    recv = refs[:n_peer]
    x_ref, n_ref, table, hits = refs[-4:]

    @pl.when(pl.program_id(0) == 0)
    def _():
        for k in range(n_peer):
            table[k * N_REQ:(k + 1) * N_REQ, :] = recv[k][...]

    ids = ids_ref[...]
    for k in range(n_peer):
        hits[:, k * N_REQ:(k + 1) * N_REQ] = (ids == gid_ref[k:k + 1, :]).astype(F32).astype(BF16)
    acc = matmul(hits[...], table[...])
    if has_prev:
        acc += refs[n_peer][...].astype(F32)
    x_ref[...] = acc.astype(BF16)
    n_ref[...] = rms_norm(acc, gain_ref[...].astype(F32)).astype(BF16)


def expand_rows(ids_col, gid, gain_row, recv, prev=None):
    n_tok, dim = ids_col.shape[0], recv[0].shape[1]
    n_peer = len(recv)
    tok = pl.BlockSpec((TOK_BLOCK, dim), lambda i: (i, 0))
    whole = pl.BlockSpec(memory_space=pltpu.VMEM)
    extra = () if prev is None else (prev,)
    return pl.pallas_call(
        functools.partial(expand_kernel, n_peer=n_peer, has_prev=prev is not None),
        grid=(n_tok // TOK_BLOCK,),
        out_shape=[jax.ShapeDtypeStruct((n_tok, dim), BF16)] * 2,
        in_specs=[pl.BlockSpec((TOK_BLOCK, 1), lambda i: (i, 0)), whole, whole] + [whole] * n_peer + [tok] * len(extra),
        out_specs=[tok, tok],
        scratch_shapes=[pltpu.VMEM((n_peer * N_REQ, dim), BF16), pltpu.VMEM((TOK_BLOCK, n_peer * N_REQ), BF16)],
        cost_estimate=pl.CostEstimate(flops=22 * 10 ** 9, bytes_accessed=30 * 10 ** 6, transcendentals=0),
        name='expand_rows',
    )(ids_col, gid, gain_row, *recv, *extra)


def hidden_kernel(n_ref, grad_ref, w_up_ref, w_dn_ref, h_ref, du_ref, u_buf, dh_buf):
    n_chunk = w_up_ref.shape[0] // F_CHUNK

    def at(c):
        return pl.ds(c * F_CHUNK if isinstance(c, int) else pl.multiple_of(c * F_CHUNK, F_CHUNK), F_CHUNK)

    def dots(c, slot):
        u_buf[slot] = contract_last(n_ref[...], w_up_ref[at(c), :])
        dh_buf[slot] = contract_last(grad_ref[...], w_dn_ref[at(c), :])

    def act(c, slot):
        u = u_buf[slot].astype(BF16).astype(F32)
        sq = u * u
        half = 0.5 * jnp.tanh(u * (GELU_A + (GELU_A * GELU_B) * sq)) + 0.5
        h_ref[:, at(c)] = (u * half).astype(BF16)
        slope = half + u * (half - half * half) * (2 * GELU_A + (6 * GELU_A * GELU_B) * sq)
        du_ref[:, at(c)] = (dh_buf[slot] * slope).astype(BF16)

    dots(0, 0)

    def pair(i, carry):
        c = 2 * i
        dots(c + 1, 1)
        act(c, 0)
        dots(c + 2, 0)
        act(c + 1, 1)
        return carry

    lax.fori_loop(0, (n_chunk - 1) // 2, pair, 0)
    act(n_chunk - 1, 0)


def hidden_arrays(normed, grad_out, w_up_t, w_dn):
    n_tok, dim = normed.shape
    ffn = w_dn.shape[0]
    tok = pl.BlockSpec((TOK_BLOCK, dim), lambda i: (i, 0))
    wide = pl.BlockSpec((TOK_BLOCK, ffn), lambda i: (i, 0))
    whole = pl.BlockSpec(memory_space=pltpu.VMEM)
    return pl.pallas_call(
        hidden_kernel,
        grid=(n_tok // TOK_BLOCK,),
        out_shape=[jax.ShapeDtypeStruct((n_tok, ffn), BF16)] * 2,
        in_specs=[tok, tok, whole, whole],
        out_specs=[wide, wide],
        scratch_shapes=[pltpu.VMEM((2, TOK_BLOCK, F_CHUNK), F32)] * 2,
        compiler_params=pltpu.CompilerParams(vmem_limit_bytes=60 * 2 ** 20),
        cost_estimate=pl.CostEstimate(flops=4 * n_tok * dim * ffn, bytes_accessed=110 * 10 ** 6, transcendentals=n_tok * ffn),
        name='hidden_arrays',
    )(normed, grad_out, w_up_t, w_dn)


def combine_kernel(gid_ref, ids_ref, dx_ref, *refs, n_out):
    dups, ones, hits = refs[:n_out], refs[n_out:2 * n_out], refs[-1]
    n_tok = dx_ref.shape[0]
    step = 1024
    for j in range(n_out):
        gid = gid_ref[j * N_REQ:(j + 1) * N_REQ, :]
        for lo in range(0, n_tok, step):
            hits[:, lo:lo + step] = (gid == ids_ref[:, lo:lo + step]).astype(F32).astype(BF16)
        acc = matmul(hits[...], dx_ref[...])
        dups[j][...] = acc[:N_DUP]
        ones[j][...] = acc[N_DUP:].astype(BF16)


def combine_rows(gid_col, ids_row, d_x):
    n_tok, dim = d_x.shape
    n_out = gid_col.shape[0] // N_REQ
    whole = pl.BlockSpec(memory_space=pltpu.VMEM)
    outs = pl.pallas_call(
        functools.partial(combine_kernel, n_out=n_out),
        out_shape=[jax.ShapeDtypeStruct((N_DUP, dim), F32)] * n_out + [jax.ShapeDtypeStruct((N_ONE, dim), BF16)] * n_out,
        in_specs=[whole, whole, whole],
        out_specs=[whole] * (2 * n_out),
        scratch_shapes=[pltpu.VMEM((N_REQ, n_tok), BF16)],
        cost_estimate=pl.CostEstimate(flops=12 * 10 ** 9, bytes_accessed=12 * 10 ** 6, transcendentals=0),
        name='combine_rows',
    )(gid_col, ids_row, d_x)
    return outs[:n_out], outs[n_out:]


def table_kernel(off_one_ref, off_dup_ref, dup_id_ref, one_id_ref, *refs, n_peer, has_prev):
    ones = refs[:n_peer]
    dups = refs[n_peer:2 * n_peer]
    out_ref, rows_buf, id_buf = refs[-3:]
    blk = pl.program_id(0)
    base = blk * V_BLOCK
    starts, trips = [], jnp.int32(1)
    for k in range(n_peer):
        lo, hi = off_one_ref[k, blk], off_one_ref[k, blk + 1]
        start = (lo // 16) * 16
        starts.append(start)
        trips = jnp.maximum(trips, jnp.where(hi > lo, (hi - start + WIN - 1) // WIN, 0))
    pos = lax.broadcasted_iota(jnp.int32, (WIN, 1), 0)
    lane = lax.broadcasted_iota(jnp.int32, (n_peer * WIN, V_BLOCK), 1) + base

    def picked(it):
        for k in range(n_peer):
            want = starts[k] + it * WIN
            at = pl.multiple_of(jnp.minimum(want, N_ONE - WIN), 16)
            rows_buf[k * WIN:(k + 1) * WIN, :] = ones[k][pl.ds(at, WIN), :]
            window = one_id_ref[pl.ds(pl.multiple_of(k * N_ONE + at, 16), WIN), :]
            id_buf[k * WIN:(k + 1) * WIN, :] = jnp.where(pos + at >= want, window, -1)
        hit = (id_buf[...] == lane).astype(F32).astype(BF16)
        return contract_first(hit, rows_buf[...])

    out_ref[...] = refs[2 * n_peer][...] + picked(0) if has_prev else picked(0)

    def one_step(it, carry):
        out_ref[...] += picked(it)
        return carry

    lax.fori_loop(1, trips, one_step, 0)
    sub = lax.broadcasted_iota(jnp.int32, (8, 1), 0)
    for k in range(n_peer):
        def dup_step(j, carry, k=k):
            row = dup_id_ref[k, j] - base
            taken = dups[k][pl.ds(pl.multiple_of((j // 8) * 8, 8), 8), :]
            taken = jnp.sum(jnp.where(sub == lax.rem(j, 8), taken, 0.0), axis=0, keepdims=True)
            at = pl.ds(pl.multiple_of((row // 8) * 8, 8), 8)
            out_ref[at, :] += jnp.where(sub == lax.rem(row, 8), taken, 0.0)
            return carry

        lax.fori_loop(off_dup_ref[k, blk], off_dup_ref[k, blk + 1], dup_step, 0)


def table_grad(vocab_local, off_one, off_dup, dup_ids, one_ids, ones, dups, prev=None):
    n_peer, dim = len(ones), ones[0].shape[1]
    n_blk = pl.cdiv(vocab_local, V_BLOCK)
    smem = pl.BlockSpec(memory_space=pltpu.SMEM)
    whole = pl.BlockSpec(memory_space=pltpu.VMEM)
    rows = pl.BlockSpec((V_BLOCK, dim), lambda b: (b, 0))
    extra = () if prev is None else (prev,)
    return pl.pallas_call(
        functools.partial(table_kernel, n_peer=n_peer, has_prev=prev is not None),
        grid=(n_blk,),
        out_shape=jax.ShapeDtypeStruct((vocab_local, dim), F32),
        in_specs=[smem, smem, smem, whole] + [whole] * (2 * n_peer) + [rows] * len(extra),
        out_specs=rows,
        scratch_shapes=[
            pltpu.VMEM((n_peer * WIN, dim), BF16),
            pltpu.VMEM((n_peer * WIN, 1), jnp.int32),
        ],
        input_output_aliases={} if prev is None else {4 + 2 * n_peer: 0},
        cost_estimate=pl.CostEstimate(flops=25 * 10 ** 9, bytes_accessed=75 * 10 ** 6, transcendentals=0),
        name='table_grad',
    )(off_one, off_dup, dup_ids, one_ids, *ones, *dups, *extra)


def solution(mesh):
    tok_spec = P(('data', 'tensor'))
    row_spec = P(('data', 'tensor'), None)
    n_peer = mesh.shape['tensor']
    swaps = [[(i, i ^ k) for i in range(n_peer)] for k in range(n_peer)]

    def exchange(k, block):
        return block if k == 0 else lax.ppermute(block, 'tensor', swaps[k])

    def local_step(token_ids, emb_shard, norm_gain, w_up, w_down, grad_out):
        vocab_local = emb_shard.shape[0]
        n_tok = token_ids.shape[0]
        me = lax.axis_index('tensor')
        peers = me ^ jnp.arange(n_peer, dtype=jnp.int32)
        w_dn = lax.all_gather(w_down, 'tensor', tiled=True)
        w_up_t = lax.all_gather(w_up.T, 'tensor', tiled=True)

        sorted_ids = jnp.sort(token_ids).reshape(n_tok // 128, 128)
        rows_of = slice(0, N_REQ // 128)

        def asked(rnd):
            mine = route(me, jnp.int32(rnd), sorted_ids, n_peer, vocab_local)
            if isinstance(rnd, int):
                theirs = swap_lists(mine)
            else:
                theirs = jnp.stack([exchange(k, mine[k]) for k in range(n_peer)])
            rounds = jnp.max(theirs[:, -1, :])
            mine, theirs = (part[:, rows_of, :].reshape(n_peer, N_REQ) for part in (mine, theirs))
            return mine, jnp.where(theirs < 0, -1, theirs - me * vocab_local), rounds

        first = asked(0)
        rounds = first[2]
        halves = (range(n_peer // 2, n_peer), range(n_peer // 2))
        ids_col, ids_row = token_ids[:, None], token_ids[None, :]
        gain_row = norm_gain[None, :]

        def lookup(lists, prev=None):
            mine, theirs, _ = lists
            idx = jnp.clip(theirs, 0, vocab_local - 1)
            recv = {}
            for half in halves:
                blocks = gather_rows(emb_shard, idx[half.start:half.stop].reshape(-1), len(half))
                recv.update({k: exchange(k, block) for k, block in zip(half, blocks)})
            return expand_rows(ids_col, mine, gain_row, [recv[k] for k in range(n_peer)], prev)

        def lookup_step(carry):
            rnd, x_prev, _ = carry
            x_new, n_new = lookup(asked(rnd), x_prev)
            return rnd + 1, x_new, n_new

        x_first, n_first = lookup(first)
        _, x_local, normed = lax.while_loop(lambda c: c[0] < rounds, lookup_step, (jnp.int32(1), x_first, n_first))

        x_f = x_local.astype(F32)
        gain_f = norm_gain.astype(F32)
        _, norm_back = jax.vjp(lambda x_in: rms_norm(x_in, gain_f), x_f)
        hidden, d_pre = hidden_arrays(normed, grad_out, w_up_t, w_dn)
        d_w_down = lax.psum_scatter(contract_first(hidden, grad_out), 'tensor', scatter_dimension=0, tiled=True)
        d_norm = matmul(d_pre, w_up_t)
        dx_local = (grad_out.astype(F32) + norm_back(d_norm)[0]).astype(BF16)
        d_w_up = lax.psum_scatter(contract_first(d_pre, normed), 'tensor', scatter_dimension=0, tiled=True).T
        out_local = (x_f + matmul(hidden, w_dn)).astype(BF16)

        def table(lists, prev=None):
            mine, theirs, _ = lists
            dups, ones = {}, {}
            for half in halves:
                gid_col = mine[half.start:half.stop].reshape(-1, 1)
                for k, dup, one in zip(half, *combine_rows(gid_col, ids_row, dx_local)):
                    ones[k], dups[k] = exchange(k, one), exchange(k, dup)
            ones, dups = ([part[k] for k in range(n_peer)] for part in (ones, dups))
            keys = jnp.where(theirs < 0, BIG, theirs)
            marks = jnp.arange(pl.cdiv(vocab_local, V_BLOCK) + 1, dtype=jnp.int32) * V_BLOCK
            offs = [jnp.sum(part[:, None, :] < marks[None, :, None], axis=-1, dtype=jnp.int32)
                    for part in (keys[:, :N_DUP], keys[:, N_DUP:])]
            return table_grad(vocab_local, offs[1], offs[0], theirs[:, :N_DUP],
                              theirs[:, N_DUP:].reshape(n_peer * N_ONE, 1), ones, dups, prev)

        def table_step(carry):
            rnd, prev = carry
            return rnd + 1, table(asked(rnd), prev)

        _, d_emb = lax.while_loop(lambda c: c[0] < rounds, table_step, (jnp.int32(1), table(first)))
        return out_local, d_emb, d_w_up, d_w_down

    return jax.shard_map(
        local_step,
        mesh=mesh,
        in_specs=(tok_spec, P('tensor', None), P(None), P(None, 'tensor'), P('tensor', None), row_spec),
        out_specs=(row_spec, row_spec, P('data', 'tensor'), row_spec),
        check_vma=False,
    )
```
